256 devices in a mesh: bank: 8 (over z_lo, y), zero: 32 (over z_hi, x, core).
Axes of the slice: x: 4, y: 4, z: 8 (z_hi: 4, z_lo: 2; z = z_hi * 2 + z_lo), core: 2. Of those that a mesh axis runs over, the one named last changes fastest.
Arguments:
- train_down: float32 [16, 6400, 4096], P('bank', None, 'zero'), may hold values from -0.15625 to 0.15625
- other_down: bfloat16 [16, 6400, 4096], P('bank', None, 'zero'), may hold values from -0.0390625 to 0.0390625
- router_weight: float32 [4096, 16], P('zero', 'bank'), may hold values from -0.09375 to 0.09375
- router_gain: float32 [4096], P('zero'), may hold values from 0.25 to 1.75
Outputs:
- ready_down: bfloat16 [16, 6400, 4096], P('bank', 'zero')
- scale_down: float32 [16, 6400], P('bank', 'zero')
- serve_router: bfloat16 [4096, 16], replicated
The draws below stay inside these ranges and needn't reach their ends.
All inputs are finite; a program needn't handle non-finite values. Where the reference program divides by a largest or mean magnitude, that divisor is 1e-20 or more.
Results may differ from the reference program's by a relative error of at most 0.001.
Values may be sent and summed in bfloat16 or wider, within the bound.
No kernel may reach another device: no remote copies, remote signals or barrier semaphores. Data moves between devices by JAX's collectives and lax.ppermute only.
A program may use at most 64 MiB of HBM per device.

```python
import jax
import jax.numpy as jnp

EXPERTS = 16
D_MODEL = 4096
D_EXPERT = 6400


def raised(values, key, source, target, shards_of, factor):
    owner, partner = [(jnp.arange(values.shape[dim]) // (values.shape[dim] // shards_of)).reshape([-1 if axis == dim else 1 for axis in range(values.ndim)]) for dim in (source, target)]
    chosen = jax.random.permutation(key, shards_of)[partner]
    strong = (owner == chosen) | (owner == (partner + shards_of // 2) % shards_of)
    return jnp.where(strong, factor * values, values)


def level_of(key, dims, cuts, least, high):
    loudness = 1.0
    for dim, blocks in cuts:
        draws = jax.random.uniform(jax.random.fold_in(jax.random.fold_in(key, 6), dim), (blocks,), jnp.float32, least / len(cuts), high / len(cuts))
        loudness = loudness * jnp.repeat(jnp.exp(draws), dims[dim] // blocks).reshape((-1,) + (1,) * (len(dims) - 1 - dim))
    return loudness


def noise(rng, dims, deviation, reach, pieces=(), held_as=jnp.bfloat16):
    result = jax.random.normal(rng, dims, jnp.float32) * deviation
    if len(pieces) > 0:
        result = level_of(rng, dims, pieces, -0.22, 0.18) * result
    return jnp.clip(result, min=-reach, max=reach).astype(held_as)


def bell_draw_with(key, extent, scale, limit, pieces, heavy, dtype=jnp.bfloat16):
    array = scale * jax.random.normal(key, extent, jnp.float32)
    if pieces:
        array = array * level_of(key, extent, pieces, -0.22, 0.18)
    return jnp.clip(raised(array, jax.random.fold_in(key, 3), *heavy), -limit, limit).astype(dtype)


def setup_inputs(seed: int = 0) -> dict:
    streams_of = jax.random.split(jax.random.key(seed), 5)
    train_down = bell_draw_with(streams_of[0], (EXPERTS, D_EXPERT, D_MODEL), D_EXPERT ** -0.5, 0.15625, ((0, 8), (2, 32)), (2, 1, 32, 2.75), jnp.float32)
    other_down = noise(streams_of[1], (EXPERTS, D_EXPERT, D_MODEL), (D_EXPERT * 4) ** -0.5, 0.0390625, ((0, 8), (2, 32)))
    router_weight = noise(streams_of[2], (D_MODEL, EXPERTS), D_MODEL ** -0.5, 0.09375, ((0, 32), (1, 8)), jnp.float32)
    router_gain = jnp.clip(1.0 + 0.15 * jax.random.normal(streams_of[3], (D_MODEL,), jnp.float32), 0.25, 1.75)
    return {"train_down": train_down, "other_down": other_down, "router_weight": router_weight, "router_gain": router_gain}


def reference(train_down, other_down, router_weight, router_gain):
    latest_down = train_down + other_down.astype(jnp.float32)
    scale_down = jnp.max(jnp.abs(latest_down), axis=2)
    ready_down = (latest_down / jnp.expand_dims(scale_down, 2)).astype(jnp.bfloat16)
    serve_router = (router_weight * router_gain[:, None]).astype(jnp.bfloat16)
    return ready_down, scale_down, serve_router
```

```python
import jax
import jax.numpy as jnp
from jax import lax
from jax.sharding import PartitionSpec as P


def from_everyone(shard, axis):
    copies = jnp.broadcast_to(shard, (lax.axis_size(axis), *shard.shape))
    return lax.all_to_all(copies, axis, split_axis=0, concat_axis=0, tiled=True)


def laid_out(tiles, dim):
    dims = list(tiles.shape[1:])
    dims[dim] *= tiles.shape[0]
    return jnp.moveaxis(tiles, 0, dim).reshape(dims)


def gathered_copies(shard, axis, dim):
    tiles = from_everyone(shard, axis)
    return laid_out(tiles, dim)


def digits(count):
    sizes = []
    while count > 1:
        sizes.append(4 if count % 4 == 0 and sizes else 2)
        count //= sizes[-1]
    return sizes


def taken_together(shard, axis):
    count = lax.axis_size(axis)
    stride = 1
    for size in digits(count):
        others = []
        for step in range(1, size):
            pairs = []
            for i in range(count):
                digit = i // stride % size
                pairs.append((i, i + ((digit + step) % size - digit) * stride))
            others.append(lax.ppermute(shard, axis, pairs))
        for other in others:
            shard = jnp.maximum(shard, other)
        stride *= size
    return shard


def local(train_down, other_down, router_weight, router_gain):
    count = lax.axis_size("zero")
    latest_down = train_down + other_down.astype(jnp.float32)
    scale_down = taken_together(jnp.max(jnp.abs(latest_down), axis=2), "zero")
    narrow_down = (latest_down / jnp.expand_dims(scale_down, 2)).astype(jnp.bfloat16)
    experts, rows, cols = narrow_down.shape
    tiles = jnp.moveaxis(narrow_down.reshape(experts, count, rows // count, cols), 1, 0)
    ready_down = laid_out(lax.all_to_all(tiles, "zero", split_axis=0, concat_axis=0, tiled=True), 2)
    scale_down = lax.dynamic_slice_in_dim(
        scale_down, lax.axis_index("zero") * ready_down.shape[1], ready_down.shape[1], axis=1
    )
    part_router = (router_weight * router_gain[:, None]).astype(jnp.bfloat16)
    row_router = gathered_copies(part_router, "zero", 0)
    serve_router = gathered_copies(row_router, "bank", 1)
    return (ready_down, scale_down, serve_router)


def solution(mesh):
    in_specs = (P("bank", None, "zero"), P("bank", None, "zero"), P("zero", "bank"), P("zero"))
    out_specs = (P("bank", "zero", None), P("bank", "zero"), P())
    return jax.shard_map(local, mesh=mesh, in_specs=in_specs, out_specs=out_specs, check_vma=False)
```
